128 devices in a mesh: band: 8 (over z, core), sector: 16 (over x, y).
Axes of the slice: x: 4, y: 4, z: 4, core: 2. Of those that a mesh axis runs over, the one named last changes fastest.
Arguments:
- node_states: bfloat16 [32, 256, 512], P('band', 'sector'), may hold values from -6 to 6
- edge_states: bfloat16 [128, 512, 512], P(('band', 'sector')), may hold values from -6 to 6
- senders: int32 [128, 512], P(('band', 'sector')), may hold values from 0 to 543, as said below
- receivers: int32 [128, 512], P(('band', 'sector')), may hold values from 0 to 63
- edge_count: int32 [128], P(('band', 'sector')), may hold values from 128 to 512, as said below
- edge_hidden: bfloat16 [2, 1536, 512], replicated, may hold values from -0.15625 to 0.15625
- edge_offset: float32 [2, 512], replicated, may hold values from -3 to 3
- edge_output: bfloat16 [2, 512, 512], replicated, may hold values from -0.25 to 0.25
- edge_scale: float32 [2, 512], replicated, may hold values from 0.5 to 1.5
- node_hidden: bfloat16 [2, 1024, 512], replicated, may hold values from -0.1875 to 0.1875
- node_offset: float32 [2, 512], replicated, may hold values from -3 to 3
- node_output: bfloat16 [2, 512, 512], replicated, may hold values from -0.25 to 0.25
- node_scale: float32 [2, 512], replicated, may hold values from 0.5 to 1.5
- output_cotangent: bfloat16 [32, 256, 512], P('band', 'sector'), may hold values from -6 to 6
Outputs:
- node_result: bfloat16 [32, 256, 512], P('band', 'sector')
- node_gradient: float32 [32, 256, 512], P('band', 'sector')
- edge_gradient: float32 [128, 512, 512], P(('band', 'sector'))
- edge_hidden_gradient: float32 [2, 1536, 512], replicated
- edge_offset_gradient: float32 [2, 512], replicated
- edge_output_gradient: float32 [2, 512, 512], replicated
- edge_scale_gradient: float32 [2, 512], replicated
- node_hidden_gradient: float32 [2, 1024, 512], replicated
- node_offset_gradient: float32 [2, 512], replicated
- node_output_gradient: float32 [2, 512, 512], replicated
- node_scale_gradient: float32 [2, 512], replicated
The draws below stay inside these ranges and needn't reach their ends.
Inputs may be any that keep to these rules, and one draw needn't show every extreme that they name: `senders`: an entry below 288 names a cell of the device's extended block (row-major, 12 rows); devices of the first band never name its first 4 rows, devices of the last band never its last 4 rows. An entry 288 + c names coarse node c. `edge_count`: slots at or past a device's count hold no edge. Some device has all 512 slots live.
All inputs are finite; a program needn't handle non-finite values.
Results may differ from the reference program's by a relative error of at most 0.019.
Values may be sent and summed in bfloat16 or wider, within the bound.
A program may use at most 128 MiB of HBM per device.

```python
import math
import jax
import jax.numpy as jnp
from jax import lax

D = 512
LB = 4
LS = 16
CO = 2
LAYERS = 2
NODE_DEV = 64
EDGE_DEV = 512
EXT = 288
COARSE = 256
NLAT = 32
NLON = 256
NODES = 8192
N_BAND = 8
N_SECTOR = 16
DEVICES = 128


def draw_senders(key, part):
    key_lat, key_lon, key_coarse, key_pick = jax.random.split(jax.random.fold_in(key, 11), 4)
    band_index = (jnp.arange(DEVICES, dtype=jnp.int32) // N_SECTOR)[:, None]
    lowest = jnp.where(band_index == 0, LB, 0).astype(jnp.int32)
    highest = jnp.where(band_index == N_BAND - 1, 2 * LB, 3 * LB).astype(jnp.int32)
    lat_pos = jax.random.randint(key_lat, (DEVICES, EDGE_DEV), lowest, highest, dtype=jnp.int32)
    lon_pos = jax.random.randint(key_lon, (DEVICES, EDGE_DEV), 0, LS + 2 * LB, dtype=jnp.int32)
    fine_index = lat_pos * (LS + 2 * LB) + lon_pos
    coarse_index = EXT + jax.random.randint(key_coarse, (DEVICES, EDGE_DEV), 0, COARSE, dtype=jnp.int32)
    picked = jax.random.randint(key_pick, (DEVICES, EDGE_DEV), 0, 4, dtype=jnp.int32) == 0
    return jnp.where(picked, coarse_index, fine_index).astype(jnp.int32)


def draw_edge_count(key, part):
    key_count, key_full = jax.random.split(jax.random.fold_in(key, 23), 2)
    counts = jax.random.randint(key_count, (DEVICES,), EDGE_DEV // 4, EDGE_DEV + 1, dtype=jnp.int32)
    fullest = jax.random.randint(key_full, (), 0, DEVICES, dtype=jnp.int32)
    return jnp.where(jnp.arange(DEVICES, dtype=jnp.int32) == fullest, EDGE_DEV, counts).astype(jnp.int32)


def place_ends(values, key, low, top_value):
    extent = values.shape
    place = [jax.random.randint(jax.random.fold_in(key, axis), (), 0, extent[axis]) for axis in range(len(extent))]
    values = values.at[tuple(place)].set(low)
    longest = extent.index(max(extent))
    place[longest] = (place[longest] + 1) % extent[longest]
    return values.at[tuple(place)].set(top_value)


def steps_of(own_key, extent, shards, low, high):
    def one(dim, blocks):
        steps = jax.random.uniform(jax.random.fold_in(jax.random.fold_in(own_key, 6), dim), (blocks,), jnp.float32, low / len(shards), high / len(shards))
        return jnp.repeat(jnp.exp(steps), extent[dim] // blocks).reshape((-1,) + (1,) * (len(extent) - dim - 1))

    loudness = one(*shards[0])
    for cut in shards[1:]:
        loudness = loudness * one(*cut)
    return loudness


def scatter_about(own_key, extent, spread, limit, pieces=(), kind=jnp.bfloat16):
    loudness = steps_of(own_key, extent, pieces, -0.22, 0.18) if pieces else 1.0
    values = jax.random.normal(own_key, extent, jnp.float32) * spread * loudness
    return jnp.minimum(jnp.maximum(values, -limit), limit).astype(kind)


def setup_inputs(seed: int = 0) -> dict:
    splits = jax.random.split(jax.random.key(seed), 15)
    node_states = scatter_about(splits[0], (NLAT, NLON, D), 1.0, 6.0, ((0, 8), (1, 16)))
    edge_states = scatter_about(splits[1], (DEVICES, EDGE_DEV, D), 1.0, 6.0, ((0, 128),))
    senders = draw_senders(jax.random.fold_in(splits[14], 71), 0)
    receivers = place_ends(jax.random.randint(splits[3], (DEVICES, EDGE_DEV), 0, NODE_DEV), jax.random.fold_in(splits[3], 1), 0, NODE_DEV - 1).astype(jnp.int32)
    edge_count = draw_edge_count(jax.random.fold_in(splits[14], 71), 0)
    edge_hidden = scatter_about(splits[5], (LAYERS, 3 * D, D), (3 * D) ** -0.5, 0.15625)
    edge_offset = scatter_about(splits[6], (LAYERS, D), 0.5, 3.0, (), jnp.float32)
    edge_output = scatter_about(splits[7], (LAYERS, D, D), D ** -0.5, 0.25)
    edge_scale = jnp.clip(1.0 + 0.1 * jax.random.normal(splits[8], (LAYERS, D), jnp.float32), 0.5, 1.5)
    node_hidden = scatter_about(splits[9], (LAYERS, 2 * D, D), (2 * D) ** -0.5, 0.1875)
    node_offset = scatter_about(splits[10], (LAYERS, D), 0.5, 3.0, (), jnp.float32)
    node_output = scatter_about(splits[11], (LAYERS, D, D), D ** -0.5, 0.25)
    node_scale = jnp.clip(1.0 + 0.1 * jax.random.normal(splits[12], (LAYERS, D), jnp.float32), 0.5, 1.5)
    output_cotangent = scatter_about(splits[13], (NLAT, NLON, D), 1.0, 6.0, ((0, 8), (1, 16)))
    return {"node_states": node_states, "edge_states": edge_states, "senders": senders, "receivers": receivers, "edge_count": edge_count, "edge_hidden": edge_hidden, "edge_offset": edge_offset, "edge_output": edge_output, "edge_scale": edge_scale, "node_hidden": node_hidden, "node_offset": node_offset, "node_output": node_output, "node_scale": node_scale, "output_cotangent": output_cotangent}


epsilon = 1e-05

def mlp_forward(inputs, first_weight, first_bias, second_weight, norm_gain):
    pre_act = jnp.dot(inputs, first_weight, preferred_element_type=jnp.float32) + first_bias
    sigmoid_val = jax.nn.sigmoid(pre_act)
    activated = (pre_act * sigmoid_val).astype(jnp.bfloat16)
    mixed = jnp.dot(activated, second_weight, preferred_element_type=jnp.float32)
    centered = mixed - lax.optimization_barrier(jnp.mean(mixed, axis=-1, keepdims=True))
    inv_std = lax.rsqrt(lax.optimization_barrier(jnp.mean(centered * centered, axis=-1, keepdims=True)) + epsilon)
    normed = centered * inv_std
    return (normed * norm_gain, (inputs, pre_act, sigmoid_val, activated, normed, inv_std))

def mlp_backward(grad_out, saved, first_weight, second_weight, norm_gain):
    inputs, pre_act, sigmoid_val, activated, normed, inv_std = saved
    grad_gain = lax.optimization_barrier(jnp.sum(grad_out * normed, axis=0))
    grad_normed = grad_out * norm_gain
    grad_mixed = inv_std * (grad_normed - lax.optimization_barrier(jnp.mean(grad_normed, axis=-1, keepdims=True)) - normed * lax.optimization_barrier(jnp.mean(grad_normed * normed, axis=-1, keepdims=True)))
    mixed_low = grad_mixed.astype(jnp.bfloat16)
    grad_second = lax.dot_general(activated, mixed_low, (((0,), (0,)), ((), ())), preferred_element_type=jnp.float32)
    grad_act = lax.dot_general(mixed_low, second_weight, (((1,), (1,)), ((), ())), preferred_element_type=jnp.float32)
    grad_pre = grad_act * sigmoid_val * (1.0 + pre_act * (1.0 - sigmoid_val))
    grad_bias = lax.optimization_barrier(jnp.sum(grad_pre, axis=0))
    pre_low = grad_pre.astype(jnp.bfloat16)
    grad_first = lax.dot_general(inputs, pre_low, (((0,), (0,)), ((), ())), preferred_element_type=jnp.float32)
    grad_inputs = lax.dot_general(pre_low, first_weight, (((1,), (1,)), ((), ())), preferred_element_type=jnp.float32)
    return (grad_inputs, (grad_first, grad_bias, grad_second, grad_gain))

def to_devices(grid):
    width = grid.shape[-1]
    return grid.reshape(N_BAND, LB, N_SECTOR, LS, width).transpose(0, 2, 1, 3, 4).reshape(DEVICES, LB * LS, width)

def to_grid(blocks):
    width = blocks.shape[-1]
    return blocks.reshape(N_BAND, N_SECTOR, LB, LS, width).transpose(0, 2, 1, 3, 4).reshape(NLAT, NLON, width)

def tables_of(state):
    padded = jnp.pad(state, ((LB, LB), (LB, LB), (0, 0)), mode='wrap')
    device_index = jnp.arange(DEVICES, dtype=jnp.int32)
    band_index = device_index // N_SECTOR
    sector_index = device_index % N_SECTOR

    def cut_block(band_pos, sector_pos):
        start = (band_pos * LB, sector_pos * LS, jnp.int32(0))
        return lax.dynamic_slice(padded, start, (3 * LB, LS + 2 * LB, D)).reshape(EXT, D)
    extended = jax.vmap(cut_block)(band_index, sector_index)
    coarse = state.reshape(N_BAND, LB, N_SECTOR, LS, D)[:, 0, :, :CO, :].reshape(COARSE, D)
    return jnp.concatenate([extended, jnp.broadcast_to(coarse, (DEVICES, COARSE, D))], axis=1)

def fold_blocks(blocks):
    blocks = blocks.reshape(DEVICES, 3 * LB, LS + 2 * LB, D)
    padded = jnp.zeros((NLAT + 2 * LB, NLON + 2 * LB, D), jnp.float32)

    def add_block(device_index, accum):
        device_index = device_index.astype(jnp.int32)
        start = (device_index // N_SECTOR * LB, device_index % N_SECTOR * LS, jnp.int32(0))
        current = lax.dynamic_slice(accum, start, (3 * LB, LS + 2 * LB, D))
        return lax.dynamic_update_slice(accum, current + blocks[device_index], start)
    padded = lax.fori_loop(jnp.int32(0), jnp.int32(DEVICES), add_block, padded)
    lon_folded = padded[:, LB:LB + NLON]
    lon_folded = lon_folded.at[:, NLON - LB:].add(padded[:, :LB]).at[:, :LB].add(padded[:, LB + NLON:])
    folded = lon_folded[LB:LB + NLAT]
    folded = folded.at[NLAT - LB:].add(lon_folded[:LB]).at[:LB].add(lon_folded[LB + NLAT:])
    return folded

def coarse_into_grid(coarse_grad):
    canvas = jnp.zeros((N_BAND, LB, N_SECTOR, LS, D), jnp.float32)
    canvas = canvas.at[:, 0, :, :CO].set(coarse_grad.reshape(N_BAND, N_SECTOR, CO, D))
    return canvas.reshape(NLAT, NLON, D)

def reference(node_states, edge_states, senders, receivers, edge_count, edge_hidden, edge_offset, edge_output, edge_scale, node_hidden, node_offset, node_output, node_scale, output_cotangent):
    live_mask = (jnp.arange(EDGE_DEV, dtype=jnp.int32)[None, :] < edge_count[:, None]).astype(jnp.float32)[:, :, None]
    device_index = jnp.arange(DEVICES, dtype=jnp.int32)[:, None]
    recv_ids = (device_index * NODE_DEV + receivers).reshape(-1)
    send_ids = (device_index * (EXT + COARSE) + senders).reshape(-1)
    state = node_states
    edge_rows = edge_states
    records = []
    for depth_index in range(LAYERS):
        tables = tables_of(state)
        own_rows = to_devices(state)
        sent = jnp.take_along_axis(tables, senders[:, :, None], axis=1)
        received = jnp.take_along_axis(own_rows, receivers[:, :, None], axis=1)
        inputs = jnp.concatenate([edge_rows, sent, received], axis=2).reshape(DEVICES * EDGE_DEV, 3 * D)
        result, edge_saved = mlp_forward(inputs, edge_hidden[depth_index], edge_offset[depth_index], edge_output[depth_index], edge_scale[depth_index])
        update = result.reshape(DEVICES, EDGE_DEV, D) * live_mask
        edge_rows = (edge_rows.astype(jnp.float32) + update).astype(jnp.bfloat16)
        summed = jax.ops.segment_sum(update.reshape(-1, D), recv_ids, num_segments=DEVICES * NODE_DEV)
        flat_rows = own_rows.reshape(-1, D)
        node_inputs = jnp.concatenate([flat_rows, summed.astype(jnp.bfloat16)], axis=1)
        node_delta, node_saved = mlp_forward(node_inputs, node_hidden[depth_index], node_offset[depth_index], node_output[depth_index], node_scale[depth_index])
        state = to_grid((flat_rows.astype(jnp.float32) + node_delta).astype(jnp.bfloat16).reshape(DEVICES, NODE_DEV, D))
        records.append((edge_saved, node_saved))
    node_result = state
    grad_grid = output_cotangent.astype(jnp.float32)
    grad_edges = jnp.zeros((DEVICES, EDGE_DEV, D), jnp.float32)
    per_layer = [None] * LAYERS
    for depth_index in reversed(range(LAYERS)):
        edge_saved, node_saved = records[depth_index]
        grad_rows = to_devices(grad_grid).reshape(-1, D)
        grad_in, node_grads = mlp_backward(grad_rows, node_saved, node_hidden[depth_index], node_output[depth_index], node_scale[depth_index])
        grad_rows = grad_rows + grad_in[:, :D]
        flow_grad = (grad_in[:, D:][recv_ids].reshape(DEVICES, EDGE_DEV, D) + grad_edges) * live_mask
        grad_inputs, edge_grads = mlp_backward(flow_grad.reshape(-1, D), edge_saved, edge_hidden[depth_index], edge_output[depth_index], edge_scale[depth_index])
        grad_inputs = grad_inputs.reshape(DEVICES, EDGE_DEV, 3 * D)
        grad_edges = grad_edges + grad_inputs[:, :, :D]
        grad_rows = grad_rows + jax.ops.segment_sum(grad_inputs[:, :, 2 * D:].reshape(-1, D), recv_ids, num_segments=DEVICES * NODE_DEV)
        table_grad = jax.ops.segment_sum(grad_inputs[:, :, D:2 * D].reshape(-1, D), send_ids, num_segments=DEVICES * (EXT + COARSE)).reshape(DEVICES, EXT + COARSE, D)
        grad_grid = to_grid(grad_rows.reshape(DEVICES, NODE_DEV, D)) + fold_blocks(table_grad[:, :EXT]) + coarse_into_grid(lax.optimization_barrier(jnp.sum(table_grad[:, EXT:], axis=0)))
        per_layer[depth_index] = edge_grads + node_grads
    factor = 1.0 / math.sqrt(NODES)
    stacked = [jnp.stack([per_layer[depth_index][item] for depth_index in range(LAYERS)]) * factor for item in range(8)]
    return (node_result, grad_grid, grad_edges, stacked[0], stacked[1], stacked[2], stacked[3], stacked[4], stacked[5], stacked[6], stacked[7])
```

```python
import functools
import math

import jax
import jax.numpy as jnp
from jax import lax
from jax.experimental import pallas as pl
from jax.experimental.pallas import tpu as pltpu
from jax.sharding import Mesh
from jax.sharding import PartitionSpec as P

AXES = ("z", "c", "x", "y")
BAND = ("z", "c")
SECTOR = ("x", "y")
ALL = ("z", "c", "x", "y")
MESH = pl.DeviceIdType.MESH
BF = jnp.bfloat16
F32 = jnp.float32
D = 512
E = 512
N = 64
TAB = 544
TR = 64
UNITS = 15
EPS = 1e-05
VMEM_LIMIT = 60 * 1024 * 1024


def iota(shape, dim):
    return lax.broadcasted_iota(jnp.int32, shape, dim)


def mm(a, b):
    return jnp.dot(a, b, preferred_element_type=F32)


def mm_tn(a, b):
    return lax.dot_general(a, b, (((0,), (0,)), ((), ())), preferred_element_type=F32)


def mm_nt(a, b):
    return lax.dot_general(a, b, (((1,), (1,)), ((), ())), preferred_element_type=F32)


def halves(v):
    hi = v.astype(BF)
    return hi, (v - hi.astype(F32)).astype(BF)


def onehot(cond):
    return jnp.where(cond, 1.0, 0.0).astype(BF)


def tiles(body, rows=E):
    def step(t, carry):
        body(pl.ds(pl.multiple_of(t * TR, TR), TR), t * TR)
        return carry

    lax.fori_loop(0, rows // TR, step, 0)


def where_am_i():
    z, c, x, y = (lax.axis_index(a) for a in AXES)
    return z, c, x, y, z * 2 + c, x * 4 + y


def device(b, s):
    return (lax.div(b, 2), lax.rem(b, 2), lax.div(s, 4), lax.rem(s, 4))


def greet(b, s):
    barrier = pltpu.get_barrier_semaphore()
    peers = [(lax.rem(b + p, 8), s) for p in range(1, 8)]
    peers += [(b, lax.rem(s + p, 16)) for p in range(1, 16)]
    peers += [(lax.rem(b + i, 8), lax.rem(s + j, 16)) for i in (1, 7) for j in (1, 15)]
    for pb, ps in peers:
        pl.semaphore_signal(barrier, inc=1, device_id=device(pb, ps), device_id_type=MESH)
    pl.semaphore_wait(barrier, len(peers))


def remote(src, dst, send, recv, dev):
    copy = pltpu.make_async_remote_copy(
        src_ref=src, dst_ref=dst, send_sem=send, recv_sem=recv, device_id=dev, device_id_type=MESH
    )
    copy.start()
    return copy


def gather_kernel(state_ref, table_ref, snd, arrived, sems):
    z, c, x, y, b, s = where_am_i()
    i = iota((112, N), 0)
    col = iota((112, N), 1)
    west = lax.div(i, 4) * 16 + lax.rem(i, 4)
    k = i - 80
    east = lax.div(k, 4) * 16 + lax.rem(k, 4) + 12
    q = i - 96
    coarse = jnp.where(lax.div(q, 2) == b, lax.rem(q, 2), -1)
    source = jnp.where(i < 16, west, jnp.where(i < 80, i - 16, jnp.where(i < 96, east, coarse)))
    picked = mm(onehot(source == col), state_ref[...]).astype(BF)
    snd[...] = picked
    table_ref[112:176, :] = state_ref[...]
    greet(b, s)
    copies = []
    for p in range(1, 8):
        copies.append(
            remote(snd.at[96:112], arrived.at[p], sems.at[0, p], sems.at[1, p], device(lax.rem(b + p, 8), s))
        )
    moves = [
        (1, 0, 16, 16, 64),
        (7, 0, 16, 208, 64),
        (0, 1, 80, 96, 16),
        (0, 15, 0, 176, 16),
        (1, 1, 80, 0, 16),
        (1, 15, 0, 80, 16),
        (7, 1, 80, 192, 16),
        (7, 15, 0, 272, 16),
    ]
    halo = []
    for m, (db, ds, src, dst, rows) in enumerate(moves):
        halo.append(
            remote(
                snd.at[src : src + rows],
                table_ref.at[dst : dst + rows],
                sems.at[2, m],
                sems.at[3, m],
                device(lax.rem(b + db, 8), lax.rem(s + ds, 16)),
            )
        )
    total = snd[96:112, :].astype(F32)
    for p in range(1, 8):
        copies[p - 1].wait_recv()
        total = total + arrived[p].astype(F32)
    mine = pl.ds(pl.multiple_of(288 + s * 16, 16), 16)
    table_ref[mine, :] = total.astype(BF)
    spread = []
    for p in range(1, 16):
        spread.append(
            remote(table_ref.at[mine], table_ref.at[mine], sems.at[4, p], sems.at[5, p], device(b, lax.rem(s + p, 16)))
        )
    for copy in copies:
        copy.wait_send()
    for copy in halo + spread:
        copy.wait()


def gather_table(state, cid):
    return pl.pallas_call(
        gather_kernel,
        name=f"gather_{cid}",
        out_shape=jax.ShapeDtypeStruct((TAB, D), BF),
        in_specs=[pl.BlockSpec(memory_space=pltpu.VMEM)],
        out_specs=pl.BlockSpec(memory_space=pltpu.VMEM),
        scratch_shapes=[
            pltpu.VMEM((112, D), BF),
            pltpu.VMEM((8, 16, D), BF),
            pltpu.SemaphoreType.DMA((6, 16)),
        ],
        compiler_params=pltpu.CompilerParams(collective_id=cid, has_side_effects=True),
    )(state)


def fold_kernel(tg_ref, part_ref, out_ref, rb, ctile, csum, atile, sems):
    z, c, x, y, b, s = where_am_i()
    greet(b, s)
    mine = pl.ds(pl.multiple_of(288 + s * 16, 16), 16)
    spread = []
    for p in range(1, 16):
        ps = lax.rem(s + p, 16)
        theirs = pl.ds(pl.multiple_of(288 + ps * 16, 16), 16)
        spread.append(remote(tg_ref.at[theirs], ctile.at[p], sems.at[0, p], sems.at[1, p], device(b, ps)))
    moves = [
        (1, 0, 208, 0, 64),
        (7, 0, 16, 64, 64),
        (0, 1, 176, 128, 16),
        (1, 1, 272, 144, 16),
        (7, 1, 80, 160, 16),
        (0, 15, 96, 176, 16),
        (1, 15, 192, 192, 16),
        (7, 15, 0, 208, 16),
    ]
    halo = []
    for m, (db, ds, src, dst, rows) in enumerate(moves):
        halo.append(
            remote(
                tg_ref.at[src : src + rows],
                rb.at[dst : dst + rows],
                sems.at[2, m],
                sems.at[3, m],
                device(lax.rem(b + db, 8), lax.rem(s + ds, 16)),
            )
        )
    total = tg_ref[mine, :].astype(F32)
    for p in range(1, 16):
        spread[p - 1].wait_recv()
        total = total + ctile[p].astype(F32)
    csum[...] = total.astype(BF)
    column = []
    for p in range(1, 8):
        column.append(remote(csum, atile.at[p], sems.at[4, p], sems.at[5, p], device(lax.rem(b + p, 8), s)))
    for copy in halo:
        copy.wait()

    def rows(at, count=16):
        return rb[at : at + count, :].astype(F32)

    west = rows(128) + rows(144) + rows(160)
    east = rows(176) + rows(192) + rows(208)
    base = part_ref[...] + rows(0, 64) + rows(64, 64)
    total = csum[...].astype(F32)
    for p in range(1, 8):
        column[p - 1].wait_recv()
        total = total + atile[p].astype(F32)
    parts = jnp.concatenate([west, east, total], axis=0)
    i = iota((N, 48), 0)
    k = iota((N, 48), 1)
    at_west = lax.div(k, 4) * 16 + lax.rem(k, 4)
    ke = k - 16
    at_east = lax.div(ke, 4) * 16 + lax.rem(ke, 4) + 12
    q = k - 32
    at_coarse = jnp.where(lax.div(q, 2) == b, lax.rem(q, 2), -1)
    place = onehot(i == jnp.where(k < 16, at_west, jnp.where(k < 32, at_east, at_coarse)))
    hi, lo = halves(parts)
    out_ref[...] = base + mm(place, hi) + mm(place, lo)
    for copy in spread + column:
        copy.wait_send()


def fold_table(tg, part, cid):
    return pl.pallas_call(
        fold_kernel,
        name=f"fold_{cid}",
        out_shape=jax.ShapeDtypeStruct((N, D), F32),
        in_specs=[pl.BlockSpec(memory_space=pltpu.VMEM)] * 2,
        out_specs=pl.BlockSpec(memory_space=pltpu.VMEM),
        scratch_shapes=[
            pltpu.VMEM((224, D), BF),
            pltpu.VMEM((16, 16, D), BF),
            pltpu.VMEM((16, D), BF),
            pltpu.VMEM((8, 16, D), BF),
            pltpu.SemaphoreType.DMA((6, 16)),
        ],
        compiler_params=pltpu.CompilerParams(collective_id=cid, has_side_effects=True),
    )(tg, part)


def activate(pre_ref, act_ref, rows):
    def body(r, start):
        p = pre_ref[r, :]
        act_ref[r, :] = (p * jax.nn.sigmoid(p)).astype(BF)

    tiles(body, rows)


def layer_norm(z):
    centered = z - jnp.mean(z, axis=-1, keepdims=True)
    inv = lax.rsqrt(jnp.mean(centered * centered, axis=-1, keepdims=True) + EPS)
    return centered * inv, inv


def forward_step(p, e_ref, table_ref, state_ref, cnt_ref, scol, rcol, rrow, s, e_new, state_new):
    xs, pre, act, n, inv, agg, npre, nact, nn, ninv, upd = s
    xs[...] = mm(onehot(iota((E, TAB), 1) == scol[...]), table_ref[...]).astype(BF)
    hi, lo = halves(mm(state_ref[...], p["eh"][0, 2 * D :, :]))
    two = jnp.concatenate([hi, lo], axis=0)
    inc2 = onehot(lax.rem(iota((E, 2 * N), 1), N) == rcol[...])
    pre[...] = (
        mm(e_ref[...], p["eh"][0, :D, :])
        + mm(xs[...], p["eh"][0, D : 2 * D, :])
        + mm(inc2, two)
        + p["eo"][...]
    )
    activate(pre, act, E)
    n[...] = mm(act[...], p["ev"][0])

    def norm(r, start):
        nrm, iv = layer_norm(n[r, :])
        n[r, :] = nrm
        inv[r, :] = jnp.broadcast_to(iv, (TR, 128))
        update = jnp.where(iota((TR, D), 0) + start < cnt_ref[0], nrm * p["es"][...], 0.0)
        upd[r, :] = update.astype(BF)
        if e_new is not None:
            e_new[r, :] = (e_ref[r, :].astype(F32) + update).astype(BF)

    tiles(norm)
    inct = onehot(iota((N, E), 0) == rrow[...])
    agg[...] = mm(inct, upd[...]).astype(BF)
    npre[...] = mm(state_ref[...], p["nh"][0, :D, :]) + mm(agg[...], p["nh"][0, D:, :]) + p["no"][...]
    activate(npre, nact, N)
    nrm, iv = layer_norm(mm(nact[...], p["nv"][0]))
    nn[...] = nrm
    ninv[...] = jnp.broadcast_to(iv, (N, 128))
    state_new[...] = (state_ref[...].astype(F32) + nrm * p["ns"][...]).astype(BF)


def put(g_ref, chunk, value):
    low = value.astype(BF)
    for lane in range(4):
        g_ref[lane // 2, 2 * chunk + lane % 2, :, :] = low[:, lane * 128 : (lane + 1) * 128]


def norm_back(u, n, inv, gain):
    dn = u * gain
    return inv * (
        dn - jnp.mean(dn, axis=-1, keepdims=True) - n * jnp.mean(dn * n, axis=-1, keepdims=True)
    )


def act_back(dact, p):
    sg = jax.nn.sigmoid(p)
    return dact * sg * (1.0 + p * (1.0 - sg))


def backward_step(
    p, e_ref, state_ref, cnt_ref, srow, rcol, rrow, s, gstate, gedge, w, g_ref, tg_ref, part_ref, gedge_out
):
    xs, pre, act, n, inv, agg, npre, nact, nn, ninv, upd = s
    big, dzb, dpb, sums = w
    u = gstate
    dzn = norm_back(u, nn[...], ninv[:, :1], p["ns"][...]).astype(BF)
    dgn = jnp.sum(u * nn[...], axis=0, keepdims=True)
    put(g_ref, 6, mm_tn(nact[...], dzn))
    dpn = act_back(mm_nt(dzn, p["nv"][0]), npre[...])
    dcn = jnp.sum(dpn, axis=0, keepdims=True)
    dpn = dpn.astype(BF)
    put(g_ref, 3, mm_tn(state_ref[...], dpn))
    put(g_ref, 4, mm_tn(agg[...], dpn))
    part = u + mm_nt(dpn, p["nh"][0, :D, :])
    hi, lo = halves(mm_nt(dpn, p["nh"][0, D:, :]))
    inc2 = onehot(lax.rem(iota((E, 2 * N), 1), N) == rcol[...])
    big[...] = mm(inc2, jnp.concatenate([hi, lo], axis=0))
    sums[...] = jnp.zeros_like(sums)

    def back(r, start):
        flow = big[r, :]
        if gedge is not None:
            flow = flow + gedge[r, :]
        flow = jnp.where(iota((TR, D), 0) + start < cnt_ref[0], flow, 0.0)
        nt = n[r, :]
        prod = flow * nt
        sums[0:8, :] += jnp.sum(prod.reshape(TR // 8, 8, D), axis=0)
        dzb[r, :] = norm_back(flow, nt, inv[r, :1], p["es"][...]).astype(BF)

    tiles(back)
    put(g_ref, 5, mm_tn(act[...], dzb[...]))
    big[...] = mm_nt(dzb[...], p["ev"][0])

    def back2(r, start):
        dp = act_back(big[r, :], pre[r, :])
        sums[8:16, :] += jnp.sum(dp.reshape(TR // 8, 8, D), axis=0)
        dpb[r, :] = dp.astype(BF)

    tiles(back2)
    put(g_ref, 0, mm_tn(e_ref[...], dpb[...]))
    put(g_ref, 1, mm_tn(xs[...], dpb[...]))
    inct = onehot(iota((N, E), 0) == rrow[...])
    tr = mm(inct, dpb[...]).astype(BF)
    put(g_ref, 2, mm_tn(state_ref[...], tr))
    part = part + mm_nt(tr, p["eh"][0, 2 * D :, :])
    de = mm_nt(dpb[...], p["eh"][0, :D, :])
    gedge_out[...] = de if gedge is None else de + gedge[...]
    xs[...] = mm_nt(dpb[...], p["eh"][0, D : 2 * D, :]).astype(BF)
    tgrad = mm(onehot(iota((TAB, E), 0) == srow[...]), xs[...])
    tg_ref[...] = tgrad.astype(BF)
    part_ref[...] = part + tgrad[112:176, :]
    dge = jnp.sum(sums[0:8, :], axis=0, keepdims=True)
    dce = jnp.sum(sums[8:16, :], axis=0, keepdims=True)
    vectors = [dce, dge, dcn, dgn]
    for core in range(2):
        g_ref[core, 14, :, :] = jnp.zeros((512, 128), BF)
        for v, vec in enumerate(vectors):
            for half in range(2):
                lane = core * 2 + half
                row = v * 2 + half
                sums[row : row + 1, 0:128] = vec[:, lane * 128 : (lane + 1) * 128]
        g_ref[core, 14, 0:8, :] = sums[0:8, 0:128].astype(BF)


WEIGHTS = ("eh", "eo", "ev", "es", "nh", "no", "nv", "ns")


def saved_shapes():
    return [
        ((E, D), BF),
        ((E, D), F32),
        ((E, D), BF),
        ((E, D), F32),
        ((E, 128), F32),
        ((N, D), BF),
        ((N, D), F32),
        ((N, D), BF),
        ((N, D), F32),
        ((N, 128), F32),
    ]


def work_shapes():
    return [((E, D), F32), ((E, D), BF), ((E, D), BF), ((16, D), F32)]


def first_kernel(*refs):
    cnt, scol, rcol, rrow, e, table, state = refs[:7]
    p = dict(zip(WEIGHTS, refs[7:15]))
    e_new, state_new = refs[15:17]
    s = refs[17:27] + (refs[27],)
    forward_step(p, e, table, state, cnt, scol, rcol, rrow, s, e_new, state_new)


def middle_kernel(*refs):
    cnt, scol, srow, rcol, rrow, e, table, state, cot = refs[:9]
    p = dict(zip(WEIGHTS, refs[9:17]))
    state_new, g_ref, tg, part, gedge = refs[17:22]
    s = refs[22:33]
    w = refs[33:37]
    forward_step(p, e, table, state, cnt, scol, rcol, rrow, s, None, state_new)
    backward_step(
        p, e, state, cnt, srow, rcol, rrow, s, cot[...].astype(F32), None, w, g_ref, tg, part, gedge
    )


def last_kernel(*refs):
    cnt, srow, rcol, rrow, e, state, gstate, gedge = refs[:8]
    s = refs[8:18]
    p = dict(zip(WEIGHTS, refs[18:26]))
    g_ref, tg, part, gedge_out = refs[26:30]
    xs = refs[30]
    w = refs[31:35]
    s = (xs,) + s[1:] + (None,)
    xs[...] = refs[8][...]
    backward_step(
        p, e, state, cnt, srow, rcol, rrow, s, gstate[...], gedge, w, g_ref, tg, part, gedge_out
    )


def vm(n):
    return [pl.BlockSpec(memory_space=pltpu.VMEM)] * n


def weight_specs(layer):
    def spec(shape):
        return pl.BlockSpec((1,) + shape, lambda i: (layer, 0, 0), pipeline_mode=pl.Buffered(1))

    return [spec(t) for t in ((3 * D, D), (1, D), (D, D), (1, D), (2 * D, D), (1, D), (D, D), (1, D))]


def squeeze_vectors(kernel, first):
    def run(*refs):
        refs = list(refs)
        for i in (1, 3, 5, 7):
            refs[first + i] = refs[first + i].at[0]
        kernel(*refs)

    return run


def full(shape):
    return pl.BlockSpec(shape, lambda i: (0,) * len(shape), pipeline_mode=pl.Buffered(1))


def compute_call(kernel, name, first, layer, small, weights, outs, scratch):
    n_before = first
    specs = [pl.BlockSpec(memory_space=pltpu.SMEM)] + [full(a.shape) for a in small[1:]]
    specs = specs[:n_before] + weight_specs(layer)
    return pl.pallas_call(
        squeeze_vectors(kernel, first),
        name=name,
        grid=(1,),
        out_shape=[jax.ShapeDtypeStruct(t, d) for t, d in outs],
        in_specs=specs,
        out_specs=[full(t) for t, d in outs],
        scratch_shapes=[pltpu.VMEM(t, d) for t, d in scratch],
        compiler_params=pltpu.CompilerParams(vmem_limit_bytes=VMEM_LIMIT),
    )(*small, *weights)


def reduce_kernel(layers, *refs):
    g = refs[:layers]
    out = refs[layers : 2 * layers]
    scratch = refs[2 * layers :]
    per = 9
    bufs = [scratch[i * per : (i + 1) * per] for i in range(layers)]
    pair_sem, ring_sem = scratch[layers * per :]
    z, c, x, y = (lax.axis_index(a) for a in AXES)
    me = {"z": z, "c": c, "x": x, "y": y}
    order = ("x", "y", "z")

    def at(**over):
        m = dict(me, **over)
        return tuple(m[a] for a in AXES)

    other = at(c=1 - c)
    barrier = pltpu.get_barrier_semaphore()
    peers = [other] + [at(**{a: lax.rem(me[a] + p, 4)}) for a in order for p in range(1, 4)]
    for peer in peers:
        pl.semaphore_signal(barrier, inc=1, device_id=peer, device_id_type=MESH)
    pl.semaphore_wait(barrier, len(peers))

    colors = [slice(5 * k, 5 * k + 5) for k in range(3)]
    sends = []

    def units(k, body):
        def step(u, carry):
            body(u)
            return carry

        lax.fori_loop(5 * k, 5 * k + 5, step, 0)

    first = {}
    for l in range(layers):
        for k in range(3):
            first[l, k] = remote(
                g[l].at[1 - c, colors[k]],
                bufs[l][0].at[colors[k]],
                pair_sem.at[0, l, k],
                pair_sem.at[1, l, k],
                other,
            )
    sends += list(first.values())
    sizes = (128, 32, 8)

    def ring(l, k, stage, src, src_rows, dst_of):
        axis = order[(k + stage) % 3]
        got = []
        for p in range(1, 4):
            to = lax.rem(me[axis] + p, 4)
            got.append(
                remote(
                    src(to),
                    dst_of(p, me[axis]),
                    ring_sem.at[0, src_rows, l, k, p],
                    ring_sem.at[1, src_rows, l, k, p],
                    at(**{axis: to}),
                )
            )
        sends.extend(got)
        return got

    inflight = {}
    for stage in range(4):
        for l in range(layers):
            r0, h0, r1, h1, r2, h2, r3, a2, a1 = bufs[l]
            received = (r1, r2, r3)
            held = (h0, h1, h2)
            for k in range(3):
                if stage == 0:
                    first[l, k].wait_recv()

                    def add(u, l=l):
                        bufs[l][1][u] = (g[l][c, u].astype(F32) + bufs[l][0][u].astype(F32)).astype(BF)

                    units(k, add)
                else:
                    for copy in inflight[l, k]:
                        copy.wait_recv()
                    axis = order[(k + stage - 1) % 3]
                    n = sizes[stage - 1]
                    src = held[stage - 1]
                    rec = received[stage - 1]
                    mine = pl.ds(pl.multiple_of(me[axis] * n, n), n)
                    if stage < 3:
                        target = held[stage]

                        def add(u, src=src, rec=rec, mine=mine, target=target):
                            v = src[u, mine, :].astype(F32)
                            for p in range(3):
                                v = v + rec[p, u].astype(F32)
                            target[u] = v.astype(BF)

                    else:
                        last = order[(k + 2) % 3]
                        spot = pl.ds(pl.multiple_of(me[last] * 8, 8), 8)

                        def add(u, src=src, rec=rec, mine=mine, spot=spot, a2=a2):
                            v = src[u, mine, :].astype(F32)
                            for p in range(3):
                                v = v + rec[p, u].astype(F32)
                            a2[u, spot, :] = v.astype(BF)

                    units(k, add)
                if stage < 3:
                    n = sizes[stage]
                    inflight[l, k] = ring(
                        l,
                        k,
                        stage,
                        lambda to, h=held[stage], n=n, k=k: h.at[colors[k], pl.ds(pl.multiple_of(to * n, n), n)],
                        stage,
                        lambda p, who, r=received[stage], k=k: r.at[p - 1, colors[k]],
                    )
                else:
                    spot = pl.ds(pl.multiple_of(me[order[(k + 2) % 3]] * 8, 8), 8)
                    inflight[l, k] = ring(
                        l,
                        k,
                        2,
                        lambda to, a2=a2, spot=spot, k=k: a2.at[colors[k], spot],
                        3,
                        lambda p, who, a2=a2, spot=spot, k=k: a2.at[colors[k], spot],
                    )
    for stage in (1, 0):
        for l in range(layers):
            a2, a1 = bufs[l][7], bufs[l][8]
            for k in range(3):
                for copy in inflight[l, k]:
                    copy.wait_recv()
                axis = order[(k + stage) % 3]
                n = sizes[stage]
                spot = pl.ds(pl.multiple_of(me[axis] * n, n), n)
                target = a1 if stage == 1 else out[l].at[c]
                source = a2 if stage == 1 else a1

                def keep(u, target=target, source=source, spot=spot):
                    target[u, spot, :] = source[u]

                units(k, keep)
                inflight[l, k] = ring(
                    l,
                    k,
                    stage,
                    lambda to, source=source, k=k: source.at[colors[k]],
                    5 - stage,
                    lambda p, who, target=target, spot=spot, k=k: target.at[colors[k], spot],
                )
    final = []
    for l in range(layers):
        for k in range(3):
            for copy in inflight[l, k]:
                copy.wait_recv()
            final.append(
                remote(
                    out[l].at[c, colors[k]],
                    out[l].at[c, colors[k]],
                    pair_sem.at[2, l, k],
                    pair_sem.at[3, l, k],
                    other,
                )
            )
    for copy in final:
        copy.wait()
    for copy in sends:
        copy.wait_send()


def sum_gradients(grads, cid):
    layers = len(grads)
    shape = (2, UNITS, 512, 128)
    per_layer = [
        pltpu.VMEM((UNITS, 512, 128), BF),
        pltpu.VMEM((UNITS, 512, 128), BF),
        pltpu.VMEM((3, UNITS, 128, 128), BF),
        pltpu.VMEM((UNITS, 128, 128), BF),
        pltpu.VMEM((3, UNITS, 32, 128), BF),
        pltpu.VMEM((UNITS, 32, 128), BF),
        pltpu.VMEM((3, UNITS, 8, 128), BF),
        pltpu.VMEM((UNITS, 32, 128), BF),
        pltpu.VMEM((UNITS, 128, 128), BF),
    ]
    return pl.pallas_call(
        functools.partial(reduce_kernel, layers),
        name=f"sum_{cid}",
        out_shape=[jax.ShapeDtypeStruct(shape, BF)] * layers,
        in_specs=vm(layers),
        out_specs=vm(layers),
        scratch_shapes=per_layer * layers
        + [pltpu.SemaphoreType.DMA((4, layers, 3)), pltpu.SemaphoreType.DMA((2, 6, layers, 3, 4))],
        compiler_params=pltpu.CompilerParams(
            collective_id=cid, has_side_effects=True, vmem_limit_bytes=VMEM_LIMIT
        ),
    )(*grads)


def widen_kernel(factor, sums_ref, eh, ev, nh, nv, vec):
    def chunk(j):
        return jnp.concatenate(
            [sums_ref[lane // 2, 2 * j + lane % 2].astype(F32) * factor for lane in range(4)], axis=1
        )

    for j in range(3):
        eh[0, j * D : (j + 1) * D, :] = chunk(j)
    for j in range(2):
        nh[0, j * D : (j + 1) * D, :] = chunk(3 + j)
    ev[0] = chunk(5)
    nv[0] = chunk(6)
    for core in range(2):
        small = sums_ref[core, 14, 0:8, :].astype(F32) * factor
        for v in range(4):
            for half in range(2):
                lane = core * 2 + half
                vec[0, v : v + 1, lane * 128 : (lane + 1) * 128] = small[v * 2 + half : v * 2 + half + 1, :]


def widen(total, layer, factor, previous):
    shapes = [(2, 3 * D, D), (2, D, D), (2, 2 * D, D), (2, D, D), (2, 4, D)]
    kernel = functools.partial(widen_kernel, factor)
    aliases = {}
    operands = (total,)
    specs = [full(total.shape)]
    if previous is not None:
        operands += tuple(previous)
        specs += [pl.BlockSpec(memory_space=pl.ANY)] * 5
        aliases = {i + 1: i for i in range(5)}
        inner = kernel

        def kernel(sums_ref, *refs):
            inner(sums_ref, *refs[5:])

    return pl.pallas_call(
        kernel,
        name=f"widen_{layer}",
        grid=(1,),
        out_shape=[jax.ShapeDtypeStruct(t, F32) for t in shapes],
        in_specs=specs,
        out_specs=[
            pl.BlockSpec((1,) + t[1:], lambda i: (layer, 0, 0), pipeline_mode=pl.Buffered(1)) for t in shapes
        ],
        input_output_aliases=aliases,
        compiler_params=pltpu.CompilerParams(vmem_limit_bytes=VMEM_LIMIT),
    )(*operands)


def local(
    node_states,
    edge_states,
    senders,
    receivers,
    edge_count,
    edge_hidden,
    edge_offset,
    edge_output,
    edge_scale,
    node_hidden,
    node_offset,
    node_output,
    node_scale,
    output_cotangent,
):
    lat, lon, width = node_states.shape
    state0 = node_states.reshape(N, D)
    cot = output_cotangent.reshape(N, D)
    e0 = edge_states[0]
    snd = senders[0]
    rcv = receivers[0]
    r = snd // 24
    cc = snd % 24
    rr = r % 4
    cell = (r // 4) * 96 + jnp.where(
        cc < 4, rr * 4 + cc, jnp.where(cc < 20, 12 + rr * 16 + cc, 60 + rr * 4 + cc)
    )
    q = snd - 288
    dev = q // 2
    far = 288 + (dev % 16) * 16 + (dev // 16) * 2 + q % 2
    place = jnp.where(snd < 288, cell, far).astype(jnp.int32)
    scol, srow = place[:, None], place[None, :]
    rcol, rrow = rcv[:, None], rcv[None, :]
    weights = (
        edge_hidden,
        edge_offset[:, None],
        edge_output,
        edge_scale[:, None],
        node_hidden,
        node_offset[:, None],
        node_output,
        node_scale[:, None],
    )
    grad_outs = [((2, UNITS, 512, 128), BF), ((TAB, D), BF), ((N, D), F32), ((E, D), F32)]

    table0 = gather_table(state0, 0)
    res = compute_call(
        first_kernel,
        "first",
        7,
        0,
        (edge_count, scol, rcol, rrow, e0, table0, state0),
        weights,
        [((E, D), BF), ((N, D), BF)] + saved_shapes(),
        [((E, D), BF)],
    )
    e1, state1 = res[:2]
    saved = res[2:]
    table1 = gather_table(state1, 1)
    result, g1, tg1, part1, gedge1 = compute_call(
        middle_kernel,
        "middle",
        9,
        1,
        (edge_count, scol, srow, rcol, rrow, e1, table1, state1, cot),
        weights,
        [((N, D), BF)] + grad_outs,
        saved_shapes() + [((E, D), BF)] + work_shapes(),
    )
    gstate1 = fold_table(tg1, part1, 2)
    g0, tg0, part0, gedge0 = compute_call(
        last_kernel,
        "last",
        18,
        0,
        (edge_count, srow, rcol, rrow, e0, state0, gstate1, gedge1) + tuple(saved),
        weights,
        grad_outs,
        [((E, D), BF)] + work_shapes(),
    )
    gstate0 = fold_table(tg0, part0, 3)
    total0, total1 = sum_gradients([g0, g1], 4)
    factor = 1.0 / math.sqrt(N * 128)
    wide = widen(total0, 0, factor, None)
    eh, ev, nh, nv, vec = widen(total1, 1, factor, wide)
    return (
        result.reshape(lat, lon, width),
        gstate0.reshape(lat, lon, width),
        gedge0[None],
        eh,
        vec[:, 0],
        ev,
        vec[:, 1],
        nh,
        vec[:, 2],
        nv,
        vec[:, 3],
    )


def solution(mesh):
    finer = Mesh(mesh.devices.reshape(4, 2, 4, 4), AXES)
    in_specs = (
        P(BAND, SECTOR, None),
        P(ALL, None, None),
        P(ALL, None),
        P(ALL, None),
        P(ALL),
        P(),
        P(),
        P(),
        P(),
        P(),
        P(),
        P(),
        P(),
        P(BAND, SECTOR, None),
    )
    out_specs = (
        P(BAND, SECTOR, None),
        P(BAND, SECTOR, None),
        P(ALL, None, None),
        P(),
        P(),
        P(),
        P(),
        P(),
        P(),
        P(),
        P(),
    )
    return jax.shard_map(local, mesh=finer, in_specs=in_specs, out_specs=out_specs, check_vma=False)
```
